32 devices in a mesh: dp: 16 (over z, x, core), mp: 2 (over y).
Axes of the slice: x: 2, y: 2, z: 4, core: 2. Of those that a mesh axis runs over, the one named last changes fastest.
Arguments:
- teacher_in: bfloat16 [16, 1024, 1408], P('dp', 'mp'), may hold values from -8 to 8
- teacher_gain: float32 [1408], replicated, may hold values from 0.5 to 1.5
- teacher_qkv: bfloat16 [3, 1408, 1408], P(None, 'mp'), may hold values from -1 to 1
- teacher_out: bfloat16 [1408, 1408], P('mp'), may hold values from -0.15625 to 0.15625
- student_in: bfloat16 [16, 1024, 1024], P('dp', None, 'mp'), may hold values from -6 to 6
- student_gain: float32 [1024], replicated, may hold values from 0.25 to 1.75
- widen_weight: bfloat16 [1024, 4096], P(None, 'mp'), may hold values from -0.1875 to 0.1875
- narrow_weight: bfloat16 [4096, 1024], P('mp'), may hold values from -0.09375 to 0.09375
- target_head: bfloat16 [1408, 1024], P('mp'), may hold values from -0.1875 to 0.1875
- positions: int32 [16, 512], P('dp'), may hold values from 0 to 1023, as said below
- counts: int32 [16], P('dp'), may hold values from 1 to 512, 4096 in all
Outputs:
- grad_widen: float32 [1024, 4096], P('dp', 'mp')
- grad_narrow: float32 [1024, 4096], P('dp', 'mp')
- losses: float32 [16], P('dp')
The draws below stay inside these ranges and needn't reach their ends.
Inputs may be any that keep to these rules, and one draw needn't show every extreme that they name: `positions`: the entries of one image's list are distinct; only the first counts of them are live. The counts of all images sum to 4096.
All inputs are finite; a program needn't handle non-finite values. No bound on the sum of `counts` on one device may be relied on, other than what follows from the above.
Results may differ from the reference program's by a relative error of at most 0.02.
Values may be sent and summed in bfloat16 or wider, within the bound.
A program may use at most 128 MiB of HBM per device.

```python
import math
import jax
import jax.numpy as jnp
import numpy as np
from jax import lax

TD = 1408
TH = 16
SD = 1024
SH = 4096
PATCHES = 1024
KEEP = 256
SLOTS = 512
IMAGES = 16
N_MP = 2


def draw_teacher_in(key, part):
    drawn = jax.random.normal(jax.random.fold_in(key, 13), (IMAGES, PATCHES, TD), jnp.float32)
    return jnp.clip(drawn, -6.0, 6.0).astype(jnp.bfloat16)


def draw_teacher_qkv(key, part):
    sigma = TD ** (-0.5)
    drawn = sigma * jax.random.normal(jax.random.fold_in(key, 24), (3, TD, TD), jnp.float32)
    return jnp.clip(drawn, -1.0, 1.0).astype(jnp.bfloat16)


def draw_positions(key, part):
    image_keys = jax.random.split(jax.random.fold_in(key, 31), IMAGES)
    return jax.vmap(lambda one_key: jax.random.permutation(one_key, PATCHES)[:SLOTS])(image_keys).astype(jnp.int32)


def shard_levels(rng, extent, shards, least, high):
    level = 1.0
    for axis_at, blocks in shards:
        heights = jax.random.uniform(jax.random.fold_in(jax.random.fold_in(rng, 6), axis_at), (blocks,), jnp.float32, least / len(shards), high / len(shards))
        level = level * jnp.repeat(jnp.exp(heights), extent[axis_at] // blocks).reshape((-1,) + (1,) * (len(extent) - 1 - axis_at))
    return level


def profile(count, total, limit, skew):
    loads = [(1 << 20) // math.isqrt(standing ** skew) + 1 for standing in range(2, count + 1)]
    rest, holding = total - limit - (count - 1), [1] * (count - 1)
    while rest > 0:
        candidates = [i for i in range(count - 1) if holding[i] < limit]
        mass, left = sum([loads[i] for i in candidates]), rest
        for i in candidates:
            more = min(limit - holding[i], max(1, left * loads[i] // mass), rest)
            holding[i] = holding[i] + more
            rest = rest - more
    return np.array([limit] + holding)


def uneven_parts(key, count, total, most, slope):
    if count == 2:
        one = jax.random.randint(key, (), max(1, total - most), min(most, total - 1) + 1)
        return jnp.stack([one, total - one])
    lengths = jnp.asarray(profile(count, total, most, slope), jnp.int32)
    pairs = (count - 1) // 2
    source_of, receiver = lengths[1:1 + 2 * pairs:2], lengths[2:2 + 2 * pairs:2]
    margin = jnp.minimum(source_of - 1, most - receiver)
    moved = jax.random.randint(jax.random.fold_in(key, 1), (pairs,), 0, 1 << 20) % (margin + 1)
    lengths = lengths.at[1:1 + 2 * pairs:2].set(source_of - moved).at[2:2 + 2 * pairs:2].set(receiver + moved)
    return lengths[jax.random.permutation(jax.random.fold_in(key, 2), count)]


def normal_values(key, shape, scale, limit, pieces=(), held_as=jnp.bfloat16):
    entries = scale * jax.random.normal(key, shape, jnp.float32)
    if pieces:
        entries = entries * shard_levels(key, shape, pieces, -0.22, 0.18)
    return jnp.clip(entries, -limit, limit).astype(held_as)


def setup_inputs(seed: int = 0) -> dict:
    keys = jax.random.split(jax.random.key(seed), 12)
    return {
        "teacher_in": draw_teacher_in(jax.random.fold_in(keys[11], 71), 0),
        "teacher_gain": jnp.clip(1.0 + 0.1 * jax.random.normal(keys[1], (TD,), jnp.float32), 0.5, 1.5),
        "teacher_qkv": draw_teacher_qkv(jax.random.fold_in(keys[11], 71), 0),
        "teacher_out": normal_values(keys[3], (TD, TD), TD ** -0.5, 0.15625, ((0, 2),)),
        "student_in": normal_values(keys[4], (IMAGES, PATCHES, SD), 1.0, 6.0, ((0, 16), (2, 2))),
        "student_gain": jnp.clip(1.0 + 0.15 * jax.random.normal(keys[5], (SD,), jnp.float32), 0.25, 1.75),
        "widen_weight": normal_values(keys[6], (SD, SH), SD ** -0.5, 0.1875, ((1, 2),)),
        "narrow_weight": normal_values(keys[7], (SH, SD), SH ** -0.5, 0.09375, ((0, 2),)),
        "target_head": normal_values(keys[8], (TD, SD), SD ** -0.5, 0.1875, ((0, 2),)),
        "positions": draw_positions(jax.random.fold_in(keys[11], 71), 0),
        "counts": uneven_parts(keys[10], IMAGES, IMAGES * KEEP, SLOTS, 2).astype(jnp.int32),
    }


EPSILON = 1e-06

def layer_norm(values, gain):
    mean_val = lax.optimization_barrier(jnp.mean(values, axis=-1, keepdims=True))
    centred = values - mean_val
    spread = lax.optimization_barrier(jnp.mean(centred * centred, axis=-1, keepdims=True))
    return centred * lax.rsqrt(spread + EPSILON) * gain

def gelu_value(pre):
    return 0.5 * pre * (1.0 + lax.erf(pre * 0.7071067811865476))

def gelu_slope(pre):
    return 0.5 * (1.0 + lax.erf(pre * 0.7071067811865476)) + pre * 0.3989422804014327 * jnp.exp(-0.5 * pre * pre)

def reference(teacher_in, teacher_gain, teacher_qkv, teacher_out, student_in, student_gain, widen_weight, narrow_weight, target_head, positions, counts):
    head_size = TD // TH
    factor = head_size ** (-0.5)
    hidden_block = SH // N_MP
    column_block = TD // N_MP
    narrow_blocks = narrow_weight.astype(jnp.float32).reshape(N_MP, hidden_block, SD)
    head_blocks = target_head.astype(jnp.float32).reshape(N_MP, column_block, SD)

    def one_image(running, inputs):
        acc_widen, acc_narrow = running
        patches, student_all, picked, live_count = inputs
        teach_normed = layer_norm(patches.astype(jnp.float32), teacher_gain).astype(jnp.bfloat16)
        key_rows = jnp.dot(teach_normed, teacher_qkv[1].T, preferred_element_type=jnp.float32).astype(jnp.bfloat16)
        value_rows = jnp.dot(teach_normed, teacher_qkv[2].T, preferred_element_type=jnp.float32).astype(jnp.bfloat16)
        query_rows = jnp.dot(teach_normed[picked], teacher_qkv[0].T, preferred_element_type=jnp.float32).astype(jnp.bfloat16)
        query_heads = query_rows.astype(jnp.float32).reshape(SLOTS, TH, head_size)
        key_heads = key_rows.astype(jnp.float32).reshape(PATCHES, TH, head_size)
        value_heads = value_rows.astype(jnp.float32).reshape(PATCHES, TH, head_size)
        scores = jnp.einsum('shd,phd->hsp', query_heads, key_heads) * factor
        largest = lax.optimization_barrier(jnp.max(scores, axis=-1, keepdims=True))
        soft_num = jnp.exp(scores - largest)
        soft_weights = (soft_num / lax.optimization_barrier(jnp.sum(soft_num, axis=-1, keepdims=True))).astype(jnp.bfloat16)
        attended = jnp.einsum('hsp,phd->shd', soft_weights.astype(jnp.float32), value_heads).astype(jnp.bfloat16).reshape(SLOTS, TD)
        blended = jnp.dot(attended, teacher_out.T, preferred_element_type=jnp.float32)
        targets = (patches[picked].astype(jnp.float32) + blended).astype(jnp.bfloat16)
        slot_ids = jnp.arange(SLOTS, dtype=jnp.int32)
        row_weight = jnp.where(slot_ids < live_count, 1.0 / live_count.astype(jnp.float32), jnp.zeros((), jnp.float32))
        student_rows = student_all[picked].astype(jnp.float32)
        normed_rows = layer_norm(student_rows, student_gain).astype(jnp.bfloat16)
        pre_act = jnp.dot(normed_rows, widen_weight, preferred_element_type=jnp.float32)
        activity = gelu_value(pre_act).astype(jnp.bfloat16)
        partials = jnp.einsum('smk,mkd->msd', activity.astype(jnp.float32).reshape(SLOTS, N_MP, hidden_block), narrow_blocks)
        partials = lax.optimization_barrier(partials.astype(jnp.bfloat16))
        branch_sum = lax.optimization_barrier(jnp.sum(partials.astype(jnp.float32), axis=0))
        outputs = (student_rows + branch_sum).astype(jnp.bfloat16)
        predicted = jnp.dot(outputs, target_head.T, preferred_element_type=jnp.float32)
        targets32 = targets.astype(jnp.float32)
        inner_sum = lax.optimization_barrier(jnp.sum(predicted * targets32, axis=-1))
        pred_sq = lax.optimization_barrier(jnp.sum(predicted * predicted, axis=-1))
        target_sq = lax.optimization_barrier(jnp.sum(targets32 * targets32, axis=-1))
        inv_pred = lax.rsqrt(pred_sq + EPSILON)
        inv_target = lax.rsqrt(target_sq + EPSILON)
        cosine = inner_sum * inv_pred * inv_target
        image_loss = jnp.sum(row_weight * (1.0 - cosine))
        pred_slope = (row_weight * cosine * inv_pred * inv_pred)[:, None] * predicted - (row_weight * inv_pred * inv_target)[:, None] * targets32
        pred_slope = pred_slope.astype(jnp.bfloat16)
        back_parts = jnp.einsum('smc,mcd->msd', pred_slope.astype(jnp.float32).reshape(SLOTS, N_MP, column_block), head_blocks)
        back_parts = lax.optimization_barrier(back_parts.astype(jnp.bfloat16))
        back_out = lax.optimization_barrier(jnp.sum(back_parts.astype(jnp.float32), axis=0)).astype(jnp.bfloat16)
        back_act = jnp.dot(back_out, narrow_weight.T, preferred_element_type=jnp.float32)
        back_pre = (back_act * gelu_slope(pre_act)).astype(jnp.bfloat16)
        acc_widen = acc_widen + jnp.dot(normed_rows.T, back_pre, preferred_element_type=jnp.float32)
        acc_narrow = acc_narrow + jnp.dot(back_out.T, activity, preferred_element_type=jnp.float32)
        return ((acc_widen, acc_narrow), image_loss)
    start_state = (jnp.zeros((SD, SH), jnp.float32), jnp.zeros((SD, SH), jnp.float32))
    (grad_widen, grad_narrow), losses = lax.scan(one_image, start_state, (teacher_in, student_in, positions, counts))
    return (grad_widen, grad_narrow, losses)
```

```python
import jax
import jax.numpy as jnp
from jax import lax
from jax.sharding import PartitionSpec as P

TD = 1408
TH = 16


EPSILON = 1e-06


def layer_norm(values, gain):
    mean_val = jnp.mean(values, axis=-1, keepdims=True)
    centred = values - mean_val
    spread = jnp.mean(centred * centred, axis=-1, keepdims=True)
    return centred * lax.rsqrt(spread + EPSILON) * gain


def gelu_value(pre):
    return 0.5 * pre * (1.0 + lax.erf(pre * 0.7071067811865476))


def gelu_slope(pre):
    return 0.5 * (1.0 + lax.erf(pre * 0.7071067811865476)) + pre * 0.3989422804014327 * jnp.exp(
        -0.5 * pre * pre
    )


def shifted(values, axis, step):
    size = lax.axis_size(axis)
    return lax.ppermute(values, axis, [((at + step) % size, at) for at in range(size)])


def peer_sum(values, axis):
    if lax.axis_size(axis) == 2:
        return values.astype(jnp.float32) + shifted(values, axis, 1).astype(jnp.float32)
    return lax.psum(values, axis).astype(jnp.float32)


def select_rows(choice, rows):
    return jnp.dot(
        choice.astype(jnp.bfloat16), rows, preferred_element_type=jnp.float32
    )


def scatter_sum(parts, axis):
    size = lax.axis_size(axis)
    own = lax.axis_index(axis)
    kept = parts.reshape((size, parts.shape[0] // size) + parts.shape[1:])
    distance = 1
    while distance < size:
        side = (own // distance) % 2
        paired = kept.reshape((kept.shape[0] // 2, 2) + kept.shape[1:])
        outgoing = lax.dynamic_index_in_dim(paired, 1 - side, 1, keepdims=False)
        staying = lax.dynamic_index_in_dim(paired, side, 1, keepdims=False)
        incoming = lax.ppermute(
            outgoing, axis, [(at, at ^ distance) for at in range(size)]
        )
        kept = staying.astype(jnp.float32) + incoming.astype(jnp.float32)
        distance *= 2
        if distance < size:
            kept = kept.astype(parts.dtype)
    return kept[0].astype(jnp.float32)


def on_device(
    teacher_in,
    teacher_gain,
    teacher_qkv,
    teacher_out,
    student_in,
    student_gain,
    widen_weight,
    narrow_weight,
    target_head,
    positions,
    counts,
):
    own_patches = teacher_in[0]
    block_rows = own_patches.shape[0]
    slot_total = positions.shape[1]
    picked = positions[0]
    live_count = counts[0]
    head_size = TD // TH
    factor = head_size ** (-0.5)
    local_width = teacher_qkv.shape[1]
    local_heads = local_width // head_size
    mp_size = lax.axis_size("mp")
    mp_index = lax.axis_index("mp")
    patch_total = block_rows * mp_size
    peer_count = lax.axis_size("dp")
    self_index = lax.axis_index("dp")

    blocks = [own_patches] + [shifted(own_patches, "mp", step) for step in range(1, mp_size)]

    every_count = lax.all_gather(counts, "dp", axis=0, tiled=True)
    order = jnp.arange(peer_count, dtype=jnp.int32)
    range_ends = jnp.sum(
        jnp.where(order[None, :] <= order[:, None], every_count[None, :], 0), axis=1
    )
    range_starts = range_ends - every_count
    own_begin = jnp.sum(jnp.where(order < self_index, every_count, 0))
    pair_width = slot_total // peer_count
    residue = jnp.mod(order - own_begin, peer_count)
    local_index = residue[:, None] + peer_count * jnp.arange(pair_width, dtype=jnp.int32)[None, :]
    send_slot = jnp.where(local_index < live_count, local_index, -1).reshape(-1)
    slot_ids = jnp.arange(slot_total, dtype=jnp.int32)
    send_choice = send_slot[:, None] == slot_ids[None, :]

    patch_ids = jnp.arange(patch_total, dtype=jnp.int32)
    student_rows = select_rows(picked[:, None] == patch_ids[None, :], student_in[0])
    sent_rows = select_rows(send_choice, student_rows.astype(jnp.bfloat16)).astype(jnp.bfloat16)
    got_rows = lax.all_to_all(
        sent_rows.reshape(peer_count, pair_width, -1), "dp", split_axis=0, concat_axis=0, tiled=True
    )
    kept_rows = slot_total // 2
    rank_list = jnp.arange(kept_rows, dtype=jnp.int32) * peer_count + self_index
    from_source = (range_starts[None, :] <= rank_list[:, None]) & (
        rank_list[:, None] < range_ends[None, :]
    )
    source_ids = jnp.sum(jnp.where(from_source, order[None, :], 0), axis=1)
    source_start = jnp.sum(jnp.where(from_source, range_starts[None, :], 0), axis=1)
    first_rank = source_start + jnp.mod(self_index - source_start, peer_count)
    flat_index = source_ids * pair_width + (rank_list - first_rank) // peer_count
    take_choice = flat_index[:, None] == slot_ids[None, : peer_count * pair_width]
    row_weight = jnp.sum(
        jnp.where(from_source, 1.0 / every_count.astype(jnp.float32)[None, :], 0.0), axis=1
    )

    own_columns = select_rows(
        take_choice, got_rows.reshape(peer_count * pair_width, -1)
    ).astype(jnp.bfloat16)
    student_width = own_columns.shape[1]
    student_full = jnp.zeros((kept_rows, student_width * mp_size), jnp.bfloat16)
    for step in range(mp_size):
        piece = own_columns if step == 0 else shifted(own_columns, "mp", step)
        student_full = lax.dynamic_update_slice_in_dim(
            student_full, piece, ((mp_index + step) % mp_size) * student_width, 1
        )
    student_f32 = student_full.astype(jnp.float32)
    normed_rows = layer_norm(student_f32, student_gain).astype(jnp.bfloat16)
    pre_act = jnp.dot(normed_rows, widen_weight, preferred_element_type=jnp.float32)
    activity = gelu_value(pre_act).astype(jnp.bfloat16)
    branch_sum = peer_sum(
        jnp.dot(activity, narrow_weight, preferred_element_type=jnp.float32).astype(jnp.bfloat16),
        "mp",
    )
    outputs = (student_f32 + branch_sum).astype(jnp.bfloat16)
    predicted = jnp.einsum("rd,cd->rc", outputs, target_head, preferred_element_type=jnp.float32)

    rolled = jnp.mod(picked - mp_index * block_rows, patch_total)
    own_start = mp_index * local_width
    key_parts, value_parts, query_in, residual = [], [], 0.0, 0.0
    for step, block in enumerate(blocks):
        normed = layer_norm(block.astype(jnp.float32), teacher_gain).astype(jnp.bfloat16)
        key_parts.append(
            jnp.einsum(
                "pi,oi->po", normed, teacher_qkv[1], preferred_element_type=jnp.float32
            ).astype(jnp.bfloat16)
        )
        value_parts.append(
            jnp.einsum(
                "pi,oi->po", normed, teacher_qkv[2], preferred_element_type=jnp.float32
            ).astype(jnp.bfloat16)
        )
        block_ids = step * block_rows + jnp.arange(block_rows, dtype=jnp.int32)
        choice = rolled[:, None] == block_ids[None, :]
        query_in = query_in + select_rows(choice, normed)
        residual = residual + select_rows(
            choice, lax.dynamic_slice_in_dim(block, own_start, local_width, 1)
        )
    query_rows = jnp.einsum(
        "si,oi->so",
        query_in.astype(jnp.bfloat16),
        teacher_qkv[0],
        preferred_element_type=jnp.float32,
    ).astype(jnp.bfloat16)
    key_rows = jnp.concatenate(key_parts, axis=0)
    value_rows = jnp.concatenate(value_parts, axis=0)
    query_heads = query_rows.reshape(slot_total, local_heads, head_size)
    key_heads = key_rows.reshape(patch_total, local_heads, head_size)
    value_heads = value_rows.reshape(patch_total, local_heads, head_size)
    scores = (
        jnp.einsum("shd,phd->hsp", query_heads, key_heads, preferred_element_type=jnp.float32)
        * factor
    )
    largest = jnp.max(scores, axis=-1, keepdims=True)
    soft_num = jnp.exp(scores - largest)
    soft_weights = (soft_num / jnp.sum(soft_num, axis=-1, keepdims=True)).astype(jnp.bfloat16)
    attended = jnp.einsum(
        "hsp,phd->shd", soft_weights, value_heads, preferred_element_type=jnp.float32
    )
    attended = attended.astype(jnp.bfloat16).reshape(slot_total, local_width)
    sent_attended = select_rows(send_choice, attended).astype(jnp.bfloat16)
    blended = select_rows(send_choice, residual.astype(jnp.bfloat16))
    for step in range(mp_size):
        piece = sent_attended if step == 0 else shifted(sent_attended, "mp", step)
        columns = lax.dynamic_slice_in_dim(
            teacher_out, ((mp_index + step) % mp_size) * local_width, local_width, 1
        )
        blended = blended + jnp.einsum(
            "sw,ow->so", piece, columns, preferred_element_type=jnp.float32
        )
    got_targets = lax.all_to_all(
        blended.astype(jnp.bfloat16).reshape(peer_count, pair_width, -1),
        "dp",
        split_axis=0,
        concat_axis=0,
        tiled=True,
    )
    targets32 = select_rows(take_choice, got_targets.reshape(peer_count * pair_width, -1))

    inner_sum, pred_sq, target_sq = peer_sum(
        jnp.stack(
            [
                jnp.sum(predicted * targets32, axis=-1),
                jnp.sum(predicted * predicted, axis=-1),
                jnp.sum(targets32 * targets32, axis=-1),
            ]
        ),
        "mp",
    )
    inv_pred = lax.rsqrt(pred_sq + EPSILON)
    inv_target = lax.rsqrt(target_sq + EPSILON)
    cosine = inner_sum * inv_pred * inv_target
    row_loss = row_weight * (1.0 - cosine)
    pred_slope = (row_weight * cosine * inv_pred * inv_pred)[:, None] * predicted - (
        row_weight * inv_pred * inv_target
    )[:, None] * targets32
    pred_slope = pred_slope.astype(jnp.bfloat16)
    back_sum = peer_sum(
        jnp.einsum("rc,cd->rd", pred_slope, target_head, preferred_element_type=jnp.float32).astype(
            jnp.bfloat16
        ),
        "mp",
    ).astype(jnp.bfloat16)
    narrow_part = jnp.einsum(
        "rd,rh->dh", back_sum, activity, preferred_element_type=jnp.float32
    ).astype(jnp.bfloat16)
    grad_narrow = scatter_sum(narrow_part, "dp")
    back_act = jnp.einsum("rd,hd->rh", back_sum, narrow_weight, preferred_element_type=jnp.float32)
    back_pre = (back_act * gelu_slope(pre_act)).astype(jnp.bfloat16)
    widen_part = jnp.einsum(
        "rd,rh->dh", normed_rows, back_pre, preferred_element_type=jnp.float32
    ).astype(jnp.bfloat16)
    grad_widen = scatter_sum(widen_part, "dp")
    source_loss = jnp.sum(jnp.where(from_source, row_loss[:, None], 0.0), axis=0)
    image_loss = scatter_sum(source_loss, "dp")
    return (grad_widen, grad_narrow, jnp.reshape(image_loss, (1,)))


def solution(mesh):
    placed = (
        P("dp", "mp", None),
        P(),
        P(None, "mp", None),
        P("mp", None),
        P("dp", None, "mp"),
        P(),
        P(None, "mp"),
        P("mp", None),
        P("mp", None),
        P("dp", None),
        P("dp"),
    )
    return jax.shard_map(
        on_device,
        mesh=mesh,
        in_specs=placed,
        out_specs=(P("dp", "mp"), P("dp", "mp"), P("dp")),
        check_vma=False,
    )
```
